32 devices in a mesh: dp: 2 (over core), expert: 4 (over y, x), mp: 4 (over z).
Axes of the slice: x: 2, y: 2, z: 4, core: 2. Of those that a mesh axis runs over, the one named last changes fastest.
Arguments:
- hidden: bfloat16 [3072, 2, 7168], P(('dp', 'expert'), None, 'mp'), may hold values from -6 to 6
- cotangent: bfloat16 [3072, 2048], P(('dp', 'expert'), 'mp'), may hold values from -6 to 6
- routes: int32 [3072, 2], P(('dp', 'expert')), may hold values from 0 to 3, all different within a row; in each aligned block of 384 rows (0 to 383, 384 to 767, ...) at most 288 rows name the same one
- combine: float32 [3072, 2], P(('dp', 'expert')), may hold values from 0.1 to 0.9
- block_pair: int32 [8, 12], P(('dp', 'expert')), may hold values from 0 to 11, each once within a row
- lengths: int32 [8, 12], P(('dp', 'expert')), may hold values from 4 to 32
- log_ratio: float32 [8, 12], P(('dp', 'expert')), may hold values from -30 to 30
Outputs:
- grad_down: float32 [4, 7168, 2048], P('expert', ('mp', 'dp'))
- expert_load: float32 [4], replicated
The draws below stay inside these ranges and needn't reach their ends.
Inputs may be any that keep to these rules, and one draw needn't show every extreme that they name: `routes`: each row names 2 different experts; in each aligned block of 384 rows (the rows of one device) no expert is named more than 288 times, and in some blocks one expert is named exactly 288 times. `block_pair`: each row holds every number of 0 to 11 once; value v marks the chosen response of the row's pair v // 2 if v is even, its rejected response if v is odd.
All inputs are finite; a program needn't handle non-finite values.
Results may differ from the reference program's by a relative error of at most 0.0029.
Values may be sent and summed in bfloat16 or wider, within the bound.
A program may use at most 128 MiB of HBM per device.

```python
import math
import jax
import jax.numpy as jnp
import numpy as np
from jax import lax

FFW = 7168
DW = 2048
EXPERTS = 4
TOP = 2
LEN = 32
PAIRS_DEV = 6
TOK_DEV = 384
MOST = 288
GROUPS = 8
TOKENS = 3072
N_DP = 2
N_EXPERT = 4


def draw_lengths(key, part):
    first, second, third = jax.random.split(jax.random.fold_in(key, 17), 3)
    lowest = LEN // 8
    blocks = 2 * PAIRS_DEV
    row_cap = jax.random.randint(first, (GROUPS, 1), lowest, LEN + 1)
    values = jax.random.randint(second, (GROUPS, blocks), lowest, row_cap + 1)
    marked = jax.random.randint(third, (), 0, GROUPS)
    values = values.at[marked, 0].set(LEN)
    values = values.at[(marked + 1) % GROUPS, 1].set(lowest)
    return values.astype(jnp.int32)


def levels(key, dims, cuts, low, high):
    loudness = 1.0
    for axis_at, shards_of in cuts:
        steps = jax.random.uniform(jax.random.fold_in(jax.random.fold_in(key, 6), axis_at), (shards_of,), jnp.float32, low / len(cuts), high / len(cuts))
        loudness = loudness * jnp.repeat(jnp.exp(steps), dims[axis_at] // shards_of).reshape((-1,) + (1,) * (len(dims) - 1 - axis_at))
    return loudness


def deal_out(own_key, own, number, rows, number_of, top, limit, slope):
    sequence = jax.random.permutation(own_key, number_of)
    heavy_load, ordinary = load_shares(number_of, rows * top, limit, slope, True), load_shares(number_of, rows * top, limit, slope, False)
    places = jnp.arange(number_of)

    def named(tallies, rotation):
        used = int((tallies > 0).sum())
        fixed = max(1, used // 4)
        passed = fixed + (places - fixed + rotation * (used - fixed)) % max(1, number_of - fixed)
        return jnp.zeros((number_of,), jnp.int32).at[sequence[jnp.where(places < fixed, places, passed)]].set(jnp.asarray(tallies, jnp.int32))

    tallies = jnp.where(number % 4 == 0, named(heavy_load, number // 4), named(ordinary, number - number // 4 - 1))
    mixed = jax.random.permutation(jax.random.fold_in(own, 3), number_of)
    donor, sink = mixed[0:number_of // 2 * 2:2], mixed[1:number_of // 2 * 2:2]
    slack = jnp.minimum(tallies[donor] - 1, limit - tallies[sink]) // 2
    slack = jnp.where((donor == sequence[0]) | (sink == sequence[0]) | (tallies[sink] == 0), 0, jnp.maximum(slack, 0))
    passed = jax.random.randint(jax.random.fold_in(own, 4), (number_of // 2,), 0, 1 << 20) % (slack + 1)
    tallies = tallies.at[donor].add(-passed).at[sink].add(passed)
    members = jnp.searchsorted(jnp.cumsum(tallies), jnp.arange(rows * top), side="right").astype(jnp.int32)
    listing = members.reshape(top, rows).T
    listing = listing[jax.random.permutation(jax.random.fold_in(own, 1), rows)]
    rotation = jax.random.randint(jax.random.fold_in(own, 2), (rows, 1), 0, top)
    return jnp.take_along_axis(listing, (jnp.arange(top)[None, :] + rotation) % top, axis=1)


def load_shares(number_of, total, limit, slope, full):
    portions = [(1 << 20) // math.isqrt(standing ** slope) + 1 for standing in range(1, number_of + 1)]
    largest = limit if full else min(limit, max(-(-total // number_of), total * portions[0] // sum(portions)))
    least = 1 if total - largest >= number_of - 1 else 0
    counts, surplus = [largest] + [least] * (number_of - 1), total - largest - least * (number_of - 1)
    while surplus > 0:
        movable = [i for i in range(1, number_of) if counts[i] < largest] or [i for i in range(1, number_of) if counts[i] < limit]
        whole, remaining = sum([portions[i] for i in movable]), surplus
        for i in movable:
            addition = min(limit - counts[i], max(1, remaining * portions[i] // whole), surplus)
            counts[i] = counts[i] + addition
            surplus = surplus - addition
    return np.array(counts)


def centred(rng, shape, scale, bound, cuts=(), held_as=jnp.bfloat16):
    level = levels(rng, shape, cuts, -0.22, 0.18) if cuts else 1.0
    values = jax.random.normal(rng, shape, jnp.float32) * scale * level
    return jnp.minimum(jnp.maximum(values, -bound), bound).astype(held_as)


def setup_inputs(seed: int = 0) -> dict:
    splits = jax.random.split(jax.random.key(seed), 8)
    hidden = centred(splits[0], (TOKENS, TOP, FFW), 1.0, 6.0, ((0, 8), (2, 4)))
    cotangent = centred(splits[1], (TOKENS, DW), 1.0, 6.0, ((0, 8), (1, 4)))
    routes_keys = jax.random.split(jax.random.fold_in(splits[2], 1), TOKENS // TOK_DEV)
    routes_turns = jax.random.permutation(jax.random.fold_in(splits[2], 3), TOKENS // TOK_DEV)
    routes = jax.vmap(lambda own, number: deal_out(jax.random.fold_in(splits[2], 2), own, number, TOK_DEV, EXPERTS, TOP, MOST, 2))(routes_keys, routes_turns).reshape((TOKENS, TOP))
    combine = jnp.clip(0.1 + 0.79999997 * jax.random.uniform(splits[3], (TOKENS, TOP), jnp.float32) ** levels(splits[3], (TOKENS, TOP), ((0, 8),), -0.2, 0.2), 0.1, 0.9)
    block_pair = jax.vmap(lambda own: jax.random.permutation(own, 2 * PAIRS_DEV))(jax.random.split(splits[4], GROUPS)).reshape((GROUPS, 2 * PAIRS_DEV)).astype(jnp.int32)
    lengths = draw_lengths(jax.random.fold_in(splits[7], 71), 0)
    log_ratio = jnp.clip(jax.random.uniform(splits[6], (GROUPS, 2 * PAIRS_DEV), jnp.float32, -30.0, 30.0) * levels(splits[6], (GROUPS, 2 * PAIRS_DEV), ((0, 8),), -0.4, 0.0), -30.0, 30.0)
    return dict(hidden=hidden, cotangent=cotangent, routes=routes, combine=combine, block_pair=block_pair, lengths=lengths, log_ratio=log_ratio)


beta_scale = 0.1


def token_weights(combine, block_pair, lengths, log_ratio, block_len):
    blocks = block_pair.shape[1]
    labels = jnp.arange(blocks, dtype=jnp.int32)
    matches = block_pair[:, :, None] == labels[None, None, :]
    by_label = jnp.sum(jnp.where(matches, log_ratio[:, :, None], 0.0), axis=1)
    margin = by_label[:, 0::2] - by_label[:, 1::2]
    pair_coef = beta_scale * jax.nn.sigmoid(-beta_scale * margin)
    owners = block_pair // 2
    pair_ids = jnp.arange(blocks // 2, dtype=jnp.int32)
    picked = owners[:, :, None] == pair_ids[None, None, :]
    block_coef = jnp.sum(jnp.where(picked, pair_coef[:, None, :], 0.0), axis=2)
    block_weight = jnp.where(block_pair % 2 == 0, -block_coef, block_coef)
    position = jnp.arange(block_len, dtype=jnp.int32)
    within = position[None, None, :] < lengths[:, :, None]
    per_token = jnp.where(within, block_weight[:, :, None], 0.0).reshape(-1)
    return combine * per_token[:, None], within.reshape(-1)


def reference(hidden, cotangent, routes, combine, block_pair, lengths, log_ratio):
    weight, within = token_weights(combine, block_pair, lengths, log_ratio, LEN)
    labels = jnp.arange(EXPERTS, dtype=jnp.int32)
    routed = routes[:, :, None] == labels[None, None, :]
    expert_load = jnp.sum(jnp.where(routed & within[:, None, None], 1.0, 0.0), axis=(0, 1)).astype(jnp.float32)
    scaled = (weight[:, :, None] * cotangent[:, None, :].astype(jnp.float32)).astype(jnp.bfloat16)
    slice_rows = TOK_DEV * N_EXPERT * TOP
    room = N_EXPERT * MOST
    hidden_rows = hidden.reshape(N_DP, slice_rows, FFW)
    scaled_rows = scaled.reshape(N_DP, slice_rows, DW)
    route_rows = routes.reshape(N_DP, slice_rows)

    def one_expert(operands, expert_idx):
        slice_hidden, slice_scaled, slice_routes = operands
        chosen = slice_routes == expert_idx
        rank_of = jnp.cumsum(chosen.astype(jnp.int32)) - 1
        target = jnp.where(chosen, rank_of, room)
        source = jnp.zeros((room,), jnp.int32).at[target].set(jnp.arange(slice_rows, dtype=jnp.int32), mode="drop")
        filled = jnp.zeros((room,), jnp.int32).at[target].set(1, mode="drop")
        packed_h = jnp.take(slice_hidden, source, axis=0).astype(jnp.float32)
        packed_s = jnp.where(filled[:, None] > 0, jnp.take(slice_scaled, source, axis=0).astype(jnp.float32), 0.0)
        return jnp.dot(packed_h.T, packed_s, preferred_element_type=jnp.float32)

    def add_slice(running, operands):
        partial_sum = lax.map(lambda expert_idx: one_expert(operands, expert_idx), labels)
        return running + partial_sum, None

    start_total = jnp.zeros((EXPERTS, FFW, DW), jnp.float32)
    grad_down, unused = lax.scan(add_slice, start_total, (hidden_rows, scaled_rows, route_rows))
    return grad_down, expert_load
```

```python
import functools

import jax
import jax.numpy as jnp
from jax import lax
from jax.experimental import pallas as pl
from jax.experimental.pallas import tpu as pltpu
from jax.sharding import PartitionSpec as P

EXP_DEV = 1
LEN = 32
LANES = 128
VMEM_ROOM = 48 * 1024 * 1024
MESH = pl.DeviceIdType.MESH


beta_scale = 0.1


def token_factors(block_pair, lengths, log_ratio, block_len):
    blocks = block_pair.shape[1]
    labels = jnp.arange(blocks, dtype=jnp.int32)
    matches = block_pair[:, :, None] == labels[None, None, :]
    by_label = jnp.sum(jnp.where(matches, log_ratio[:, :, None], 0.0), axis=1)
    margin = by_label[:, 0::2] - by_label[:, 1::2]
    pair_coef = beta_scale * jax.nn.sigmoid(-beta_scale * margin)
    owners = block_pair // 2
    pair_ids = jnp.arange(blocks // 2, dtype=jnp.int32)
    picked = owners[:, :, None] == pair_ids[None, None, :]
    block_coef = jnp.sum(jnp.where(picked, pair_coef[:, None, :], 0.0), axis=2)
    block_weight = jnp.where(block_pair % 2 == 0, -block_coef, block_coef)
    position = jnp.arange(block_len, dtype=jnp.int32)
    within = position[None, None, :] < lengths[:, :, None]
    per_token = jnp.where(within, block_weight[:, :, None], 0.0).reshape(-1)
    return per_token, within.reshape(-1)


def exchange_kernel(
    dims, h_ref, cot_ref, routes_ref, flat_ref, weight_ref, live_ref,
    hr, sa, sb, load_ref,
    hs, sas, sbs, cotb, lbuf,
    xa_s, a_r, up_s, dn_s, dd_s, cb_s, cb_r, xb_s, b_r, db_s, h_s, h_r, l_s, l_r,
):
    nd, ne, nm, most, ca, cb = dims
    d, e, m = lax.axis_index("dp"), lax.axis_index("expert"), lax.axis_index("mp")
    toks, ff = h_ref.shape[0] // 2, h_ref.shape[1]
    half = ff // nd
    me = d * ne + e

    def dev(dd=None, ee=None, mm=None):
        return {"dp": d if dd is None else dd, "expert": e if ee is None else ee, "mp": m if mm is None else mm}

    def remote(src, dst, ssem, rsem, where):
        return pltpu.make_async_remote_copy(
            src_ref=src, dst_ref=dst, send_sem=ssem, recv_sem=rsem, device_id=where, device_id_type=MESH
        )

    barrier = pltpu.get_barrier_semaphore()
    peers = [
        dev(dd=lax.rem(d + i, nd), ee=lax.rem(e + j, ne)) for i in range(nd) for j in range(ne) if i or j
    ] + [dev(mm=lax.rem(m + i, nm)) for i in range(1, nm)]
    for peer in peers:
        pl.semaphore_signal(barrier, inc=1, device_id=peer, device_id_type=MESH)

    def ranks(named, n):
        before = lax.broadcasted_iota(jnp.int32, (n, n), 0) < lax.broadcasted_iota(jnp.int32, (n, n), 1)
        rank = jnp.dot(
            jnp.where(named, 1.0, 0.0).astype(jnp.bfloat16),
            jnp.where(before, 1.0, 0.0).astype(jnp.bfloat16),
            preferred_element_type=jnp.float32,
        )
        return jnp.where(named, rank, -1.0).astype(jnp.int32)

    rows8 = -(-ne // 8) * 8
    row_id = lax.broadcasted_iota(jnp.int32, (rows8, 1), 0)
    owner = jnp.where(row_id < ne, lax.rem(row_id + e, ne), -1)
    hit0 = routes_ref[0:1, :] == owner
    hit1 = routes_ref[1:2, :] == owner
    named = hit0 | hit1
    tok_pos = ranks(named, toks)
    tok_weight = jnp.where(hit0, weight_ref[0:1, :], 0.0) + jnp.where(hit1, weight_ref[1:2, :], 0.0)
    in_order = (routes_ref[0:1, :] == row_id) | (routes_ref[1:2, :] == row_id)
    counts = jnp.sum(jnp.where(in_order, live_ref[...], 0.0), axis=1, keepdims=True)
    lbuf[me] = jnp.broadcast_to(counts, (rows8, LANES))

    slot_tok = lax.broadcasted_iota(jnp.int32, (most, toks), 0)
    picks, scales = [], []
    for j in range(ne):
        hit = slot_tok == tok_pos[j : j + 1, :]
        picks.append(jnp.where(hit, 1.0, 0.0).astype(jnp.bfloat16))
        scales.append(jnp.sum(jnp.where(hit, tok_weight[j : j + 1, :], 0.0), axis=1, keepdims=True))

    def pack_s(j, rows):
        rows = jnp.dot(picks[j], rows, preferred_element_type=jnp.float32)
        return (scales[j] * rows).astype(jnp.bfloat16)

    sends = []
    for j in range(ne):
        block = pack_s(j, cot_ref[:, :ca])
        if j == 0:
            sa[m, me] = block
        else:
            sas[j] = block
    cotb[m] = cot_ref[:, ca:]

    pl.semaphore_wait(barrier, len(peers))

    for j in range(1, ne):
        copy = remote(sas.at[j], sa.at[m, me], xa_s.at[j], a_r.at[m, me], dev(ee=lax.rem(e + j, ne)))
        copy.start()
        sends.append(copy)
    for i in range(1, nm):
        copy = remote(cot_ref.at[:, pl.ds(ca, cb)], cotb.at[m], cb_s.at[i], cb_r.at[m], dev(mm=lax.rem(m + i, nm)))
        copy.start()
        sends.append(copy)
    n = 0
    for i in range(nd):
        for j in range(ne):
            if i or j:
                copy = remote(
                    lbuf.at[me], lbuf.at[me], l_s.at[n], l_r.at[me], dev(dd=lax.rem(d + i, nd), ee=lax.rem(e + j, ne))
                )
                copy.start()
                sends.append(copy)
                n += 1

    guarded = []

    def forward(q, src, up, down, ek):
        block = sa.at[q, src]
        cu = remote(block, block, up_s.at[q, ek], a_r.at[q, src], dev(mm=lax.rem(m + 1, nm)))
        cd = remote(block, block, dn_s.at[q, ek], a_r.at[q, src], dev(mm=lax.rem(m + nm - 1, nm)))

        @pl.when(up)
        def _():
            cu.start()

        @pl.when(down)
        def _():
            cd.start()

        guarded.append((up, cu))
        guarded.append((down, cd))

    def to_partners(q, src, ek, guard=None):
        for i in range(1, nd):
            c = remote(sa.at[q, src], sa.at[q, src], dd_s.at[q, i - 1, ek], a_r.at[q, src], dev(dd=lax.rem(d + i, nd)))
            if guard is None:
                c.start()
                sends.append(c)
            else:
                pl.when(guard)(c.start)
                guarded.append((guard, c))

    forward(m, me, m + 1 < nm, m > 0, e)
    to_partners(m, me, e)

    slot_flat = lax.broadcasted_iota(jnp.int32, (most, 2 * toks), 0)
    flat_pos = ranks(flat_ref[...] == owner, 2 * toks)
    for j in [*range(1, ne), 0]:
        pick = jnp.where(slot_flat == flat_pos[j : j + 1, :], 1.0, 0.0).astype(jnp.bfloat16)
        for c in range(nd):
            cols = pl.ds(c * half, half)
            hs[j, c] = jnp.dot(pick, h_ref[:, cols], preferred_element_type=jnp.float32).astype(jnp.bfloat16)
        for i in range(nd):
            to = lax.rem(d + i, nd)
            if i or j:
                copy = remote(
                    hs.at[j, to], hr.at[me], h_s.at[j, i], h_r.at[me], dev(dd=to, ee=lax.rem(e + j, ne))
                )
                copy.start()
                sends.append(copy)
    hr[me] = hs[0, d]

    def wait_in(buf, sem, guard=None):
        c = pltpu.make_async_copy(buf, buf, sem)
        if guard is None:
            c.wait()
        else:
            pl.when(guard)(c.wait)

    for i in range(1, nm):
        q = lax.rem(m + i, nm)
        wait_in(cotb.at[q], cb_r.at[q])
    dense = jnp.concatenate([cotb[q] for q in range(nm)], axis=1)
    for j in range(ne):
        block = pack_s(j, dense)
        if j == 0:
            sb[me] = block
            for i in range(1, nd):
                copy = remote(sb.at[me], sb.at[me], db_s.at[i - 1, 0], b_r.at[me], dev(dd=lax.rem(d + i, nd)))
                copy.start()
                sends.append(copy)
        else:
            sbs[j] = block
            copy = remote(sbs.at[j], sb.at[me], xb_s.at[j], b_r.at[me], dev(ee=lax.rem(e + j, ne)))
            copy.start()
            sends.append(copy)

    for j in range(1, ne):
        ej = lax.rem(e + j, ne)
        src = d * ne + ej
        wait_in(sa.at[m, src], a_r.at[m, src])
        forward(m, src, m + 1 < nm, m > 0, ej)
        to_partners(m, src, ej)
    for k in range(1, nm):
        below, above = m - k, m + k
        ql, qh = lax.rem(below + nm, nm), lax.rem(above, nm)
        never = m < 0
        for j in range(ne):
            ej = lax.rem(e + j, ne)
            src = d * ne + ej
            wait_in(sa.at[ql, src], a_r.at[ql, src], below >= 0)
            c = remote(sa.at[ql, src], sa.at[ql, src], up_s.at[ql, ej], a_r.at[ql, src], dev(mm=lax.rem(m + 1, nm)))
            go = (below >= 0) & (m + 1 < nm)
            pl.when(go)(c.start)
            guarded.append((go, c))
            to_partners(ql, src, ej, below >= 0)
            wait_in(sa.at[qh, src], a_r.at[qh, src], above < nm)
            c = remote(sa.at[qh, src], sa.at[qh, src], dn_s.at[qh, ej], a_r.at[qh, src], dev(mm=lax.rem(m + nm - 1, nm)))
            go = (above < nm) & (m > 0)
            pl.when(go)(c.start)
            guarded.append((go, c))
            to_partners(qh, src, ej, above < nm)

    for j in range(1, ne):
        src = d * ne + lax.rem(e + j, ne)
        wait_in(sb.at[src], b_r.at[src])
        for i in range(1, nd):
            copy = remote(sb.at[src], sb.at[src], db_s.at[i - 1, j], b_r.at[src], dev(dd=lax.rem(d + i, nd)))
            copy.start()
            sends.append(copy)

    for i in range(1, nd):
        other = lax.rem(d + i, nd)
        for j in range(ne):
            src = other * ne + j
            wait_in(sb.at[src], b_r.at[src])
            for q in range(nm):
                wait_in(sa.at[q, src], a_r.at[q, src])
    for i in range(nd):
        for j in range(ne):
            if i or j:
                src = lax.rem(d + i, nd) * ne + lax.rem(e + j, ne)
                wait_in(hr.at[src], h_r.at[src])
                wait_in(lbuf.at[src], l_r.at[src])
    total = lbuf[0]
    for k in range(1, nd * ne):
        total = total + lbuf[k]
    load_ref[...] = total

    for c in sends:
        c.wait_send()
    for go, c in guarded:
        pl.when(go)(c.wait_send)


def product_kernel(h_ref, sa_ref, sb_ref, out_ref, turned):
    @pl.when(pl.program_id(0) == 0)
    def _():
        turned[...] = h_ref[...].T

    rows = jnp.concatenate([sa_ref[0], sb_ref[...]], axis=1)
    out_ref[0] = jnp.dot(turned[...], rows, preferred_element_type=jnp.float32)


def fast_body(hidden, cotangent, routes, combine, block_pair, lengths, log_ratio):
    nd, ne, nm = lax.axis_size("dp"), lax.axis_size("expert"), lax.axis_size("mp")
    per_token, within = token_factors(block_pair, lengths, log_ratio, LEN)
    toks, top, ff = hidden.shape
    width = cotangent.shape[1]
    most = 3 * toks // 4
    cb = width // 4 // LANES * LANES
    ca = width - cb
    half = ff // nd
    srcs = nd * ne
    rows8 = -(-ne // 8) * 8
    dims = (nd, ne, nm, most, ca, cb)
    bf16, f32 = jnp.bfloat16, jnp.float32
    routes_t = routes.T
    weight_t = combine.T * per_token[None, :]
    live = jnp.where(within, 1.0, 0.0).astype(f32)[None, :]
    vmem = pl.BlockSpec(memory_space=pltpu.VMEM)
    dma = pltpu.SemaphoreType.DMA
    hr, sa, sb, load = pl.pallas_call(
        functools.partial(exchange_kernel, dims),
        out_shape=(
            jax.ShapeDtypeStruct((srcs, most, half), bf16),
            jax.ShapeDtypeStruct((nm, srcs, most, ca), bf16),
            jax.ShapeDtypeStruct((srcs, most, nm * cb), bf16),
            jax.ShapeDtypeStruct((rows8, LANES), f32),
        ),
        in_specs=[vmem] * 6,
        out_specs=(vmem,) * 4,
        scratch_shapes=[
            pltpu.VMEM((ne, nd, most, half), bf16),
            pltpu.VMEM((ne, most, ca), bf16),
            pltpu.VMEM((ne, most, nm * cb), bf16),
            pltpu.VMEM((nm, toks, cb), bf16),
            pltpu.VMEM((srcs, rows8, LANES), f32),
            dma((ne,)),
            dma((nm, srcs)),
            dma((nm, ne)),
            dma((nm, ne)),
            dma((nm, nd, ne)),
            dma((nm,)),
            dma((nm,)),
            dma((ne,)),
            dma((srcs,)),
            dma((nd, ne)),
            dma((ne, nd)),
            dma((srcs,)),
            dma((srcs,)),
            dma((srcs,)),
        ],
        compiler_params=pltpu.CompilerParams(
            collective_id=0, has_side_effects=True, vmem_limit_bytes=VMEM_ROOM
        ),
    )(hidden.reshape(toks * top, ff), cotangent, routes_t, routes.reshape(1, toks * top), weight_t, live)
    depth = srcs * most
    grad_down = pl.pallas_call(
        product_kernel,
        out_shape=jax.ShapeDtypeStruct((1, half, nm * width), f32),
        grid=(nm,),
        in_specs=[
            pl.BlockSpec((depth, half), lambda q: (0, 0)),
            pl.BlockSpec((1, depth, ca), lambda q: (q, 0, 0)),
            pl.BlockSpec((depth, cb), lambda q: (0, q)),
        ],
        out_specs=pl.BlockSpec((1, half, width), lambda q: (0, 0, q)),
        scratch_shapes=[pltpu.VMEM((half, depth), bf16)],
        compiler_params=pltpu.CompilerParams(vmem_limit_bytes=VMEM_ROOM),
    )(hr.reshape(depth, half), sa.reshape(nm, depth, ca), sb.reshape(depth, nm * cb))
    return grad_down, load[:ne, 0]


def plain_body(hidden, cotangent, routes, combine, block_pair, lengths, log_ratio):
    per_token, within = token_factors(block_pair, lengths, log_ratio, LEN)
    weight = combine * per_token[:, None]
    tok_rows = routes.shape[0]
    route_top = routes.shape[1]
    ff_local = hidden.shape[2]
    groups = lax.axis_size("expert")
    experts = groups * EXP_DEV
    most_rows = 3 * tok_rows // 4
    labels = jnp.arange(experts, dtype=jnp.int32)
    routed = routes[:, :, None] == labels[None, None, :]
    local_load = jnp.sum(jnp.where(routed & within[:, None, None], 1.0, 0.0), axis=(0, 1)).astype(
        jnp.float32
    )
    flat_rows = tok_rows * route_top
    flat_hits = routed.reshape(flat_rows, experts).astype(jnp.int32)
    rank_of = jnp.sum((jnp.cumsum(flat_hits, axis=0) - 1) * flat_hits, axis=1)
    slot_of = routes.reshape(flat_rows) * most_rows + rank_of
    source = (
        jnp.zeros((experts * most_rows,), jnp.int32)
        .at[slot_of]
        .set(jnp.arange(flat_rows, dtype=jnp.int32))
    )
    filled = jnp.zeros((experts * most_rows,), jnp.float32).at[slot_of].set(1.0)
    token_of = source // route_top
    slot_weight = jnp.take(weight.reshape(flat_rows), source) * filled
    packed_h = jnp.take(hidden.reshape(flat_rows, ff_local), source, axis=0).reshape(
        groups, EXP_DEV * most_rows, ff_local
    )
    narrow_s = (
        slot_weight[:, None] * jnp.take(cotangent, token_of, axis=0).astype(jnp.float32)
    ).astype(jnp.bfloat16)
    moved_h, narrow = (
        lax.all_to_all(packed_h, "expert", split_axis=0, concat_axis=0, tiled=True),
        lax.all_to_all(
            narrow_s.reshape(groups, EXP_DEV * most_rows, cotangent.shape[1]),
            "expert",
            split_axis=0,
            concat_axis=0,
            tiled=True,
        ),
    )
    moved_s = lax.all_gather(narrow, "mp", axis=2, tiled=True)
    moved_h = moved_h.reshape(groups, EXP_DEV, most_rows, ff_local)
    moved_s = moved_s.reshape(groups, EXP_DEV, most_rows, moved_s.shape[2])
    products = [
        lax.dot_general(
            moved_h[:, 0],
            moved_s[:, 0],
            (((0, 1), (0, 1)), ((), ())),
            preferred_element_type=jnp.float32,
        )
    ]
    owned = lax.psum_scatter(jnp.stack(products, axis=1), "dp", scatter_dimension=0, tiled=True)
    grad_down = jnp.transpose(owned, (1, 0, 2))
    expert_load = lax.psum(local_load, ("dp", "expert"))
    return (grad_down, expert_load)


def solution(mesh):
    in_specs = (
        P(("dp", "expert"), None, "mp"),
        P(("dp", "expert"), "mp"),
        P(("dp", "expert"), None),
        P(("dp", "expert"), None),
        P(("dp", "expert"), None),
        P(("dp", "expert"), None),
        P(("dp", "expert"), None),
    )
    out_specs = (P("expert", ("mp", "dp"), None), P())

    def body(hidden, cotangent, *rest):
        rows = mesh.shape["dp"] * mesh.shape["expert"] * (3 * hidden.shape[0] // 4)
        bytes_in = 2 * rows * (cotangent.shape[1] * mesh.shape["mp"] + hidden.shape[2])
        run = fast_body if 2 * bytes_in < VMEM_ROOM else plain_body
        return run(hidden, cotangent, *rest)

    return jax.shard_map(body, mesh=mesh, in_specs=in_specs, out_specs=out_specs, check_vma=False)
```

```python
import functools

import jax
import jax.numpy as jnp
from jax import lax
from jax.experimental import pallas as pl
from jax.experimental.pallas import tpu as pltpu
from jax.sharding import PartitionSpec as P

EXP_DEV = 1
LEN = 32
LANES = 128
VMEM_ROOM = 48 * 1024 * 1024
MESH = pl.DeviceIdType.MESH


beta_scale = 0.1


def token_factors(block_pair, lengths, log_ratio, block_len):
    blocks = block_pair.shape[1]
    labels = jnp.arange(blocks, dtype=jnp.int32)
    matches = block_pair[:, :, None] == labels[None, None, :]
    by_label = jnp.sum(jnp.where(matches, log_ratio[:, :, None], 0.0), axis=1)
    margin = by_label[:, 0::2] - by_label[:, 1::2]
    pair_coef = beta_scale * jax.nn.sigmoid(-beta_scale * margin)
    owners = block_pair // 2
    pair_ids = jnp.arange(blocks // 2, dtype=jnp.int32)
    picked = owners[:, :, None] == pair_ids[None, None, :]
    block_coef = jnp.sum(jnp.where(picked, pair_coef[:, None, :], 0.0), axis=2)
    block_weight = jnp.where(block_pair % 2 == 0, -block_coef, block_coef)
    position = jnp.arange(block_len, dtype=jnp.int32)
    within = position[None, None, :] < lengths[:, :, None]
    per_token = jnp.where(within, block_weight[:, :, None], 0.0).reshape(-1)
    return per_token, within.reshape(-1)


def exchange_kernel(
    dims, h_hbm, cot_hbm, routes_hbm, combine_hbm, pair_hbm, len_hbm, ratio_hbm,
    hr, sa, sb, load_ref,
    h_in, cot_ref, routes_ref, combine_ref, pair_ref, len_ref, ratio_ref,
    hs, sas, sbs, cotb, lbuf, in_sem,
    xa_s, a_r, up_s, dn_s, dd_s, cb_s, cb_r, xb_s, b_r, db_s, h_s, h_r, l_s, l_r,
):
    nd, ne, nm, most, ca, cb = dims
    d, e, m = lax.axis_index("dp"), lax.axis_index("expert"), lax.axis_index("mp")
    toks, top, ff = h_in.shape
    half = ff // nd
    me = d * ne + e

    def dev(dd=None, ee=None, mm=None):
        return {"dp": d if dd is None else dd, "expert": e if ee is None else ee, "mp": m if mm is None else mm}

    def remote(src, dst, ssem, rsem, where):
        return pltpu.make_async_remote_copy(
            src_ref=src, dst_ref=dst, send_sem=ssem, recv_sem=rsem, device_id=where, device_id_type=MESH
        )

    loads = [
        pltpu.make_async_copy(src, dst, in_sem.at[i])
        for i, (src, dst) in enumerate((
            (pair_hbm, pair_ref), (len_hbm, len_ref), (ratio_hbm, ratio_ref), (routes_hbm, routes_ref),
            (combine_hbm, combine_ref), (cot_hbm, cot_ref), (h_hbm, h_in),
        ))
    ]
    for load in loads:
        load.start()
    barrier = pltpu.get_barrier_semaphore()
    peers = [
        dev(dd=lax.rem(d + i, nd), ee=lax.rem(e + j, ne)) for i in range(nd) for j in range(ne) if i or j
    ] + [dev(mm=lax.rem(m + i, nm)) for i in range(1, nm)]
    for peer in peers:
        pl.semaphore_signal(barrier, inc=1, device_id=peer, device_id_type=MESH)

    def ranks(named, n):
        before = lax.broadcasted_iota(jnp.int32, (n, n), 0) < lax.broadcasted_iota(jnp.int32, (n, n), 1)
        rank = jnp.dot(
            jnp.where(named, 1.0, 0.0).astype(jnp.bfloat16),
            jnp.where(before, 1.0, 0.0).astype(jnp.bfloat16),
            preferred_element_type=jnp.float32,
        )
        return jnp.where(named, rank, -1.0)

    for load in loads[:-1]:
        load.wait()

    blocks = pair_ref.shape[1]
    block_len = toks // blocks
    square = (blocks, blocks)
    diagonal = lax.broadcasted_iota(jnp.int32, square, 0) == lax.broadcasted_iota(jnp.int32, square, 1)

    def column(row):
        return jnp.sum(jnp.where(diagonal, row, 0.0), axis=1, keepdims=True)

    pair, ratio = pair_ref[...], ratio_ref[...]
    chosen = lax.rem(pair, 2) == 0
    other_side = jnp.where(chosen, pair + 1, pair - 1)
    is_other = column(pair.astype(jnp.float32)) == other_side.astype(jnp.float32)
    other_ratio = jnp.sum(jnp.where(is_other, column(ratio), 0.0), axis=0, keepdims=True)
    margin = jnp.where(chosen, ratio - other_ratio, other_ratio - ratio)
    coef = beta_scale * (1.0 / (1.0 + jnp.exp(beta_scale * margin)))
    block_weight = column(jnp.where(chosen, -coef, coef))
    token_id = lax.broadcasted_iota(jnp.int32, (blocks, toks), 1)
    place = token_id - block_len * lax.broadcasted_iota(jnp.int32, (blocks, toks), 0)
    inside = (place >= 0) & (place < block_len)
    alive = inside & (place.astype(jnp.float32) < column(len_ref[...].astype(jnp.float32)))
    live = jnp.sum(jnp.where(alive, 1.0, 0.0), axis=0, keepdims=True)
    per_token = jnp.sum(jnp.where(alive, block_weight, 0.0), axis=0, keepdims=True)
    weight = combine_ref[...] * per_token

    rows8 = -(-ne // 8) * 8
    row_id = lax.broadcasted_iota(jnp.int32, (rows8, 1), 0)
    owner = jnp.where(row_id < ne, lax.rem(row_id + e, ne), -1)
    hit0 = routes_ref[0:1, :] == owner
    hit1 = routes_ref[1:2, :] == owner
    named = hit0 | hit1
    tok_rank = ranks(named, toks)
    tok_pos = tok_rank.astype(jnp.int32)
    tok_weight = jnp.where(hit0, weight[0:1, :], 0.0) + jnp.where(hit1, weight[1:2, :], 0.0)
    in_order = (routes_ref[0:1, :] == row_id) | (routes_ref[1:2, :] == row_id)
    counts = jnp.sum(jnp.where(in_order, live, 0.0), axis=1, keepdims=True)
    lbuf[me] = jnp.broadcast_to(counts, (rows8, LANES))

    slot_tok = lax.broadcasted_iota(jnp.int32, (most, toks), 0)
    picks, scales = [], []
    for j in range(ne):
        hit = slot_tok == tok_pos[j : j + 1, :]
        picks.append(jnp.where(hit, 1.0, 0.0).astype(jnp.bfloat16))
        scales.append(jnp.sum(jnp.where(hit, tok_weight[j : j + 1, :], 0.0), axis=1, keepdims=True))

    def pack_s(j, rows):
        rows = jnp.dot(picks[j], rows, preferred_element_type=jnp.float32)
        return (scales[j] * rows).astype(jnp.bfloat16)

    sends = []
    for j in range(ne):
        block = pack_s(j, cot_ref[:, :ca])
        if j == 0:
            sa[m, me] = block
        else:
            sas[j] = block
    cotb[m] = cot_ref[:, ca:]

    pl.semaphore_wait(barrier, len(peers))

    for j in range(1, ne):
        copy = remote(sas.at[j], sa.at[m, me], xa_s.at[j], a_r.at[m, me], dev(ee=lax.rem(e + j, ne)))
        copy.start()
        sends.append(copy)
    for i in range(1, nm):
        copy = remote(cot_ref.at[:, pl.ds(ca, cb)], cotb.at[m], cb_s.at[i], cb_r.at[m], dev(mm=lax.rem(m + i, nm)))
        copy.start()
        sends.append(copy)
    n = 0
    for i in range(nd):
        for j in range(ne):
            if i or j:
                copy = remote(
                    lbuf.at[me], lbuf.at[me], l_s.at[n], l_r.at[me], dev(dd=lax.rem(d + i, nd), ee=lax.rem(e + j, ne))
                )
                copy.start()
                sends.append(copy)
                n += 1

    guarded = []

    def forward(q, src, up, down, ek):
        block = sa.at[q, src]
        cu = remote(block, block, up_s.at[q, ek], a_r.at[q, src], dev(mm=lax.rem(m + 1, nm)))
        cd = remote(block, block, dn_s.at[q, ek], a_r.at[q, src], dev(mm=lax.rem(m + nm - 1, nm)))

        @pl.when(up)
        def _():
            cu.start()

        @pl.when(down)
        def _():
            cd.start()

        guarded.append((up, cu))
        guarded.append((down, cd))

    def to_partners(q, src, ek, guard=None):
        for i in range(1, nd):
            c = remote(sa.at[q, src], sa.at[q, src], dd_s.at[q, i - 1, ek], a_r.at[q, src], dev(dd=lax.rem(d + i, nd)))
            if guard is None:
                c.start()
                sends.append(c)
            else:
                pl.when(guard)(c.start)
                guarded.append((guard, c))

    forward(m, me, m + 1 < nm, m > 0, e)
    to_partners(m, me, e)

    slot_flat = lax.broadcasted_iota(jnp.int32, (most, 2 * toks), 0)
    gap = lax.broadcasted_iota(jnp.int32, (toks, 2 * toks), 1) - 2 * lax.broadcasted_iota(
        jnp.int32, (toks, 2 * toks), 0
    )
    flat_pos = -1.0
    for k, hit in enumerate((hit0, hit1)):
        spread = jnp.where(gap == k, 1.0, 0.0).astype(jnp.bfloat16)
        value = jnp.where(hit, tok_rank + 1.0, 0.0)
        high = jnp.floor(value * (1.0 / 16.0))
        for part, unit in ((high, 16.0), (value - 16.0 * high, 1.0)):
            flat_pos += unit * jnp.dot(part.astype(jnp.bfloat16), spread, preferred_element_type=jnp.float32)
    flat_pos = flat_pos.astype(jnp.int32)
    loads[-1].wait()
    flat = (2 * toks, half)
    h_rows = [h_in[:, :, c * half : (c + 1) * half].reshape(flat) for c in range(nd)]
    for j in [*range(1, ne), 0]:
        pick = jnp.where(slot_flat == flat_pos[j : j + 1, :], 1.0, 0.0).astype(jnp.bfloat16)
        for c in range(nd):
            hs[j, c] = jnp.dot(pick, h_rows[c], preferred_element_type=jnp.float32).astype(jnp.bfloat16)
        for i in range(nd):
            to = lax.rem(d + i, nd)
            if i or j:
                copy = remote(
                    hs.at[j, to], hr.at[me], h_s.at[j, i], h_r.at[me], dev(dd=to, ee=lax.rem(e + j, ne))
                )
                copy.start()
                sends.append(copy)
    hr[me] = hs[0, d]

    def wait_in(buf, sem, guard=None):
        c = pltpu.make_async_copy(buf, buf, sem)
        if guard is None:
            c.wait()
        else:
            pl.when(guard)(c.wait)

    for i in range(1, nm):
        q = lax.rem(m + i, nm)
        wait_in(cotb.at[q], cb_r.at[q])
    dense = jnp.concatenate([cotb[q] for q in range(nm)], axis=1)
    for j in range(ne):
        block = pack_s(j, dense)
        if j == 0:
            sb[me] = block
            for i in range(1, nd):
                copy = remote(sb.at[me], sb.at[me], db_s.at[i - 1, 0], b_r.at[me], dev(dd=lax.rem(d + i, nd)))
                copy.start()
                sends.append(copy)
        else:
            sbs[j] = block
            copy = remote(sbs.at[j], sb.at[me], xb_s.at[j], b_r.at[me], dev(ee=lax.rem(e + j, ne)))
            copy.start()
            sends.append(copy)

    for j in range(1, ne):
        ej = lax.rem(e + j, ne)
        src = d * ne + ej
        wait_in(sa.at[m, src], a_r.at[m, src])
        forward(m, src, m + 1 < nm, m > 0, ej)
        to_partners(m, src, ej)
    for k in range(1, nm):
        below, above = m - k, m + k
        ql, qh = lax.rem(below + nm, nm), lax.rem(above, nm)
        never = m < 0
        for j in range(ne):
            ej = lax.rem(e + j, ne)
            src = d * ne + ej
            wait_in(sa.at[ql, src], a_r.at[ql, src], below >= 0)
            c = remote(sa.at[ql, src], sa.at[ql, src], up_s.at[ql, ej], a_r.at[ql, src], dev(mm=lax.rem(m + 1, nm)))
            go = (below >= 0) & (m + 1 < nm)
            pl.when(go)(c.start)
            guarded.append((go, c))
            to_partners(ql, src, ej, below >= 0)
            wait_in(sa.at[qh, src], a_r.at[qh, src], above < nm)
            c = remote(sa.at[qh, src], sa.at[qh, src], dn_s.at[qh, ej], a_r.at[qh, src], dev(mm=lax.rem(m + nm - 1, nm)))
            go = (above < nm) & (m > 0)
            pl.when(go)(c.start)
            guarded.append((go, c))
            to_partners(qh, src, ej, above < nm)

    for j in range(1, ne):
        src = d * ne + lax.rem(e + j, ne)
        wait_in(sb.at[src], b_r.at[src])
        for i in range(1, nd):
            copy = remote(sb.at[src], sb.at[src], db_s.at[i - 1, j], b_r.at[src], dev(dd=lax.rem(d + i, nd)))
            copy.start()
            sends.append(copy)

    for i in range(1, nd):
        other = lax.rem(d + i, nd)
        for j in range(ne):
            src = other * ne + j
            wait_in(sb.at[src], b_r.at[src])
            for q in range(nm):
                wait_in(sa.at[q, src], a_r.at[q, src])
    for i in range(nd):
        for j in range(ne):
            if i or j:
                src = lax.rem(d + i, nd) * ne + lax.rem(e + j, ne)
                wait_in(hr.at[src], h_r.at[src])
                wait_in(lbuf.at[src], l_r.at[src])
    total = lbuf[0]
    for k in range(1, nd * ne):
        total = total + lbuf[k]
    load_ref[...] = total

    for c in sends:
        c.wait_send()
    for go, c in guarded:
        pl.when(go)(c.wait_send)


def product_kernel(h_ref, sa_ref, sb_ref, out_ref, turned):
    @pl.when(pl.program_id(0) == 0)
    def _():
        turned[...] = h_ref[...].T

    rows = jnp.concatenate([sa_ref[0], sb_ref[...]], axis=1)
    out_ref[0] = jnp.dot(turned[...], rows, preferred_element_type=jnp.float32)


def fast_body(hidden, cotangent, routes, combine, block_pair, lengths, log_ratio):
    nd, ne, nm = lax.axis_size("dp"), lax.axis_size("expert"), lax.axis_size("mp")
    toks, top, ff = hidden.shape
    width = cotangent.shape[1]
    most = 3 * toks // 4
    cb = width // 4 // LANES * LANES
    ca = width - cb
    half = ff // nd
    srcs = nd * ne
    rows8 = -(-ne // 8) * 8
    dims = (nd, ne, nm, most, ca, cb)
    bf16, f32 = jnp.bfloat16, jnp.float32
    vmem = pl.BlockSpec(memory_space=pltpu.VMEM)
    dma = pltpu.SemaphoreType.DMA
    hr, sa, sb, load = pl.pallas_call(
        functools.partial(exchange_kernel, dims),
        out_shape=(
            jax.ShapeDtypeStruct((srcs, most, half), bf16),
            jax.ShapeDtypeStruct((nm, srcs, most, ca), bf16),
            jax.ShapeDtypeStruct((srcs, most, nm * cb), bf16),
            jax.ShapeDtypeStruct((rows8, LANES), f32),
        ),
        in_specs=[pl.BlockSpec(memory_space=pltpu.HBM)] * 7,
        out_specs=(vmem,) * 4,
        scratch_shapes=[
            pltpu.VMEM((toks, top, ff), bf16),
            pltpu.VMEM(cotangent.shape, bf16),
            pltpu.VMEM((top, toks), jnp.int32),
            pltpu.VMEM((top, toks), f32),
            pltpu.VMEM(block_pair.shape, jnp.int32),
            pltpu.VMEM(lengths.shape, jnp.int32),
            pltpu.VMEM(log_ratio.shape, f32),
            pltpu.VMEM((ne, nd, most, half), bf16),
            pltpu.VMEM((ne, most, ca), bf16),
            pltpu.VMEM((ne, most, nm * cb), bf16),
            pltpu.VMEM((nm, toks, cb), bf16),
            pltpu.VMEM((srcs, rows8, LANES), f32),
            dma((7,)),
            dma((ne,)),
            dma((nm, srcs)),
            dma((nm, ne)),
            dma((nm, ne)),
            dma((nm, nd, ne)),
            dma((nm,)),
            dma((nm,)),
            dma((ne,)),
            dma((srcs,)),
            dma((nd, ne)),
            dma((ne, nd)),
            dma((srcs,)),
            dma((srcs,)),
            dma((srcs,)),
        ],
        compiler_params=pltpu.CompilerParams(
            collective_id=0, has_side_effects=True, vmem_limit_bytes=VMEM_ROOM
        ),
    )(hidden, cotangent, routes.T, combine.T, block_pair, lengths, log_ratio)
    depth = srcs * most
    grad_down = pl.pallas_call(
        product_kernel,
        out_shape=jax.ShapeDtypeStruct((1, half, nm * width), f32),
        grid=(nm,),
        in_specs=[
            pl.BlockSpec((depth, half), lambda q: (0, 0)),
            pl.BlockSpec((1, depth, ca), lambda q: (q, 0, 0)),
            pl.BlockSpec((depth, cb), lambda q: (0, q)),
        ],
        out_specs=pl.BlockSpec((1, half, width), lambda q: (0, 0, q)),
        scratch_shapes=[pltpu.VMEM((half, depth), bf16)],
        compiler_params=pltpu.CompilerParams(vmem_limit_bytes=VMEM_ROOM),
    )(hr.reshape(depth, half), sa.reshape(nm, depth, ca), sb.reshape(depth, nm * cb))
    return grad_down, load[:ne, 0]


def plain_body(hidden, cotangent, routes, combine, block_pair, lengths, log_ratio):
    per_token, within = token_factors(block_pair, lengths, log_ratio, LEN)
    weight = combine * per_token[:, None]
    tok_rows = routes.shape[0]
    route_top = routes.shape[1]
    ff_local = hidden.shape[2]
    groups = lax.axis_size("expert")
    experts = groups * EXP_DEV
    most_rows = 3 * tok_rows // 4
    labels = jnp.arange(experts, dtype=jnp.int32)
    routed = routes[:, :, None] == labels[None, None, :]
    local_load = jnp.sum(jnp.where(routed & within[:, None, None], 1.0, 0.0), axis=(0, 1)).astype(
        jnp.float32
    )
    flat_rows = tok_rows * route_top
    flat_hits = routed.reshape(flat_rows, experts).astype(jnp.int32)
    rank_of = jnp.sum((jnp.cumsum(flat_hits, axis=0) - 1) * flat_hits, axis=1)
    slot_of = routes.reshape(flat_rows) * most_rows + rank_of
    source = (
        jnp.zeros((experts * most_rows,), jnp.int32)
        .at[slot_of]
        .set(jnp.arange(flat_rows, dtype=jnp.int32))
    )
    filled = jnp.zeros((experts * most_rows,), jnp.float32).at[slot_of].set(1.0)
    token_of = source // route_top
    slot_weight = jnp.take(weight.reshape(flat_rows), source) * filled
    packed_h = jnp.take(hidden.reshape(flat_rows, ff_local), source, axis=0).reshape(
        groups, EXP_DEV * most_rows, ff_local
    )
    narrow_s = (
        slot_weight[:, None] * jnp.take(cotangent, token_of, axis=0).astype(jnp.float32)
    ).astype(jnp.bfloat16)
    moved_h, narrow = (
        lax.all_to_all(packed_h, "expert", split_axis=0, concat_axis=0, tiled=True),
        lax.all_to_all(
            narrow_s.reshape(groups, EXP_DEV * most_rows, cotangent.shape[1]),
            "expert",
            split_axis=0,
            concat_axis=0,
            tiled=True,
        ),
    )
    moved_s = lax.all_gather(narrow, "mp", axis=2, tiled=True)
    moved_h = moved_h.reshape(groups, EXP_DEV, most_rows, ff_local)
    moved_s = moved_s.reshape(groups, EXP_DEV, most_rows, moved_s.shape[2])
    products = [
        lax.dot_general(
            moved_h[:, 0],
            moved_s[:, 0],
            (((0, 1), (0, 1)), ((), ())),
            preferred_element_type=jnp.float32,
        )
    ]
    owned = lax.psum_scatter(jnp.stack(products, axis=1), "dp", scatter_dimension=0, tiled=True)
    grad_down = jnp.transpose(owned, (1, 0, 2))
    expert_load = lax.psum(local_load, ("dp", "expert"))
    return (grad_down, expert_load)


def solution(mesh):
    in_specs = (
        P(("dp", "expert"), None, "mp"),
        P(("dp", "expert"), "mp"),
        P(("dp", "expert"), None),
        P(("dp", "expert"), None),
        P(("dp", "expert"), None),
        P(("dp", "expert"), None),
        P(("dp", "expert"), None),
    )
    out_specs = (P("expert", ("mp", "dp"), None), P())

    def body(hidden, cotangent, *rest):
        rows = mesh.shape["dp"] * mesh.shape["expert"] * (3 * hidden.shape[0] // 4)
        bytes_in = 2 * rows * (cotangent.shape[1] * mesh.shape["mp"] + hidden.shape[2])
        run = fast_body if 2 * bytes_in < VMEM_ROOM else plain_body
        return run(hidden, cotangent, *rest)

    return jax.shard_map(body, mesh=mesh, in_specs=in_specs, out_specs=out_specs, check_vma=False)
```

```python
import functools

import jax
import jax.numpy as jnp
from jax import lax
from jax.experimental import pallas as pl
from jax.experimental.pallas import tpu as pltpu
from jax.sharding import PartitionSpec as P

EXP_DEV = 1
LEN = 32
LANES = 128
VMEM_ROOM = 48 * 1024 * 1024
VMEM_MOST = 67043328
MESH = pl.DeviceIdType.MESH


beta_scale = 0.1


def token_factors(block_pair, lengths, log_ratio, block_len):
    blocks = block_pair.shape[1]
    labels = jnp.arange(blocks, dtype=jnp.int32)
    matches = block_pair[:, :, None] == labels[None, None, :]
    by_label = jnp.sum(jnp.where(matches, log_ratio[:, :, None], 0.0), axis=1)
    margin = by_label[:, 0::2] - by_label[:, 1::2]
    pair_coef = beta_scale * jax.nn.sigmoid(-beta_scale * margin)
    owners = block_pair // 2
    pair_ids = jnp.arange(blocks // 2, dtype=jnp.int32)
    picked = owners[:, :, None] == pair_ids[None, None, :]
    block_coef = jnp.sum(jnp.where(picked, pair_coef[:, None, :], 0.0), axis=2)
    block_weight = jnp.where(block_pair % 2 == 0, -block_coef, block_coef)
    position = jnp.arange(block_len, dtype=jnp.int32)
    within = position[None, None, :] < lengths[:, :, None]
    per_token = jnp.where(within, block_weight[:, :, None], 0.0).reshape(-1)
    return per_token, within.reshape(-1)


def exchange_kernel(
    dims, h_hbm, cot_hbm, routes_hbm, combine_hbm, pair_hbm, len_hbm, ratio_hbm,
    ht_out, acc_out, last_out, sb_out, load_ref,
    h_in, cot_ref, routes_ref, combine_ref, pair_ref, len_ref, ratio_ref,
    hr, sa, sb, ht, stage,
    hs, sas, sbs, cotb, lbuf, in_sem, out_sem,
    xa_s, a_r, up_s, dn_s, dd_s, cb_s, cb_r, xb_s, b_r, db_s, h_s, h_r, l_s, l_r,
):
    nd, ne, nm, most, ca, cb = dims
    d, e, m = lax.axis_index("dp"), lax.axis_index("expert"), lax.axis_index("mp")
    toks, top, ff = h_in.shape
    half = ff // nd
    me = d * ne + e

    def dev(dd=None, ee=None, mm=None):
        return {"dp": d if dd is None else dd, "expert": e if ee is None else ee, "mp": m if mm is None else mm}

    def remote(src, dst, ssem, rsem, where):
        return pltpu.make_async_remote_copy(
            src_ref=src, dst_ref=dst, send_sem=ssem, recv_sem=rsem, device_id=where, device_id_type=MESH
        )

    loads = [
        pltpu.make_async_copy(src, dst, in_sem.at[i])
        for i, (src, dst) in enumerate((
            (pair_hbm, pair_ref), (len_hbm, len_ref), (ratio_hbm, ratio_ref), (routes_hbm, routes_ref),
            (combine_hbm, combine_ref), (cot_hbm, cot_ref), (h_hbm, h_in),
        ))
    ]
    for load in loads:
        load.start()
    barrier = pltpu.get_barrier_semaphore()
    peers = [
        dev(dd=lax.rem(d + i, nd), ee=lax.rem(e + j, ne)) for i in range(nd) for j in range(ne) if i or j
    ] + [dev(mm=lax.rem(m + i, nm)) for i in range(1, nm)]
    for peer in peers:
        pl.semaphore_signal(barrier, inc=1, device_id=peer, device_id_type=MESH)

    def ranks(named, n):
        before = lax.broadcasted_iota(jnp.int32, (n, n), 0) < lax.broadcasted_iota(jnp.int32, (n, n), 1)
        rank = jnp.dot(
            jnp.where(named, 1.0, 0.0).astype(jnp.bfloat16),
            jnp.where(before, 1.0, 0.0).astype(jnp.bfloat16),
            preferred_element_type=jnp.float32,
        )
        return jnp.where(named, rank, -1.0)

    for load in loads[:-1]:
        load.wait()

    blocks = pair_ref.shape[1]
    block_len = toks // blocks
    square = (blocks, blocks)
    diagonal = lax.broadcasted_iota(jnp.int32, square, 0) == lax.broadcasted_iota(jnp.int32, square, 1)

    def column(row):
        return jnp.sum(jnp.where(diagonal, row, 0.0), axis=1, keepdims=True)

    pair, ratio = pair_ref[...], ratio_ref[...]
    chosen = lax.rem(pair, 2) == 0
    other_side = jnp.where(chosen, pair + 1, pair - 1)
    is_other = column(pair.astype(jnp.float32)) == other_side.astype(jnp.float32)
    other_ratio = jnp.sum(jnp.where(is_other, column(ratio), 0.0), axis=0, keepdims=True)
    margin = jnp.where(chosen, ratio - other_ratio, other_ratio - ratio)
    coef = beta_scale * (1.0 / (1.0 + jnp.exp(beta_scale * margin)))
    block_weight = column(jnp.where(chosen, -coef, coef))
    token_id = lax.broadcasted_iota(jnp.int32, (blocks, toks), 1)
    place = token_id - block_len * lax.broadcasted_iota(jnp.int32, (blocks, toks), 0)
    inside = (place >= 0) & (place < block_len)
    alive = inside & (place.astype(jnp.float32) < column(len_ref[...].astype(jnp.float32)))
    live = jnp.sum(jnp.where(alive, 1.0, 0.0), axis=0, keepdims=True)
    per_token = jnp.sum(jnp.where(alive, block_weight, 0.0), axis=0, keepdims=True)
    weight = combine_ref[...] * per_token

    rows8 = -(-ne // 8) * 8
    row_id = lax.broadcasted_iota(jnp.int32, (rows8, 1), 0)
    owner = jnp.where(row_id < ne, lax.rem(row_id + e, ne), -1)
    hit0 = routes_ref[0:1, :] == owner
    hit1 = routes_ref[1:2, :] == owner
    named = hit0 | hit1
    tok_rank = ranks(named, toks)
    tok_pos = tok_rank.astype(jnp.int32)
    tok_weight = jnp.where(hit0, weight[0:1, :], 0.0) + jnp.where(hit1, weight[1:2, :], 0.0)
    in_order = (routes_ref[0:1, :] == row_id) | (routes_ref[1:2, :] == row_id)
    counts = jnp.sum(jnp.where(in_order, live, 0.0), axis=1, keepdims=True)
    lanes8 = lax.broadcasted_iota(jnp.int32, (rows8, LANES), 1) == row_id
    lbuf[me] = jnp.broadcast_to(jnp.sum(jnp.where(lanes8, counts, 0.0), axis=0, keepdims=True), (rows8, LANES))

    slot_tok = lax.broadcasted_iota(jnp.int32, (most, toks), 0)
    picks, scales = [], []
    for j in range(ne):
        hit = slot_tok == tok_pos[j : j + 1, :]
        picks.append(jnp.where(hit, 1.0, 0.0).astype(jnp.bfloat16))
        scales.append(jnp.sum(jnp.where(hit, tok_weight[j : j + 1, :], 0.0), axis=1, keepdims=True))

    def pack_s(j, rows):
        rows = jnp.dot(picks[j], rows, preferred_element_type=jnp.float32)
        return (scales[j] * rows).astype(jnp.bfloat16)

    sends = []
    for j in range(ne):
        block = pack_s(j, cot_ref[:, :ca])
        if j == 0:
            sa[m, me] = block
        else:
            sas[j] = block
    cotb[m] = cot_ref[:, ca:]

    pl.semaphore_wait(barrier, len(peers))

    for j in range(1, ne):
        copy = remote(sas.at[j], sa.at[m, me], xa_s.at[j], a_r.at[m, me], dev(ee=lax.rem(e + j, ne)))
        copy.start()
        sends.append(copy)
    for i in range(1, nm):
        copy = remote(cot_ref.at[:, pl.ds(ca, cb)], cotb.at[m], cb_s.at[i], cb_r.at[m], dev(mm=lax.rem(m + i, nm)))
        copy.start()
        sends.append(copy)
    n = 0
    for i in range(nd):
        for j in range(ne):
            if i or j:
                copy = remote(
                    lbuf.at[me], lbuf.at[me], l_s.at[n], l_r.at[me], dev(dd=lax.rem(d + i, nd), ee=lax.rem(e + j, ne))
                )
                copy.start()
                sends.append(copy)
                n += 1

    guarded = []

    def forward(q, src, up, down, ek):
        block = sa.at[q, src]
        cu = remote(block, block, up_s.at[q, ek], a_r.at[q, src], dev(mm=lax.rem(m + 1, nm)))
        cd = remote(block, block, dn_s.at[q, ek], a_r.at[q, src], dev(mm=lax.rem(m + nm - 1, nm)))

        @pl.when(up)
        def _():
            cu.start()

        @pl.when(down)
        def _():
            cd.start()

        guarded.append((up, cu))
        guarded.append((down, cd))

    def to_partners(q, src, ek, guard=None):
        for i in range(1, nd):
            c = remote(sa.at[q, src], sa.at[q, src], dd_s.at[q, i - 1, ek], a_r.at[q, src], dev(dd=lax.rem(d + i, nd)))
            if guard is None:
                c.start()
                sends.append(c)
            else:
                pl.when(guard)(c.start)
                guarded.append((guard, c))

    forward(m, me, m + 1 < nm, m > 0, e)
    to_partners(m, me, e)

    slot_flat = lax.broadcasted_iota(jnp.int32, (most, 2 * toks), 0)
    gap = lax.broadcasted_iota(jnp.int32, (toks, 2 * toks), 1) - 2 * lax.broadcasted_iota(
        jnp.int32, (toks, 2 * toks), 0
    )
    flat_pos = -1.0
    for k, hit in enumerate((hit0, hit1)):
        spread = jnp.where(gap == k, 1.0, 0.0).astype(jnp.bfloat16)
        value = jnp.where(hit, tok_rank + 1.0, 0.0)
        high = jnp.floor(value * (1.0 / 16.0))
        for part, unit in ((high, 16.0), (value - 16.0 * high, 1.0)):
            flat_pos += unit * jnp.dot(part.astype(jnp.bfloat16), spread, preferred_element_type=jnp.float32)
    flat_pos = flat_pos.astype(jnp.int32)
    loads[-1].wait()
    flat = (2 * toks, half)
    h_rows = [h_in[:, :, c * half : (c + 1) * half].reshape(flat) for c in range(nd)]
    for j in [*range(1, ne), 0]:
        pick = jnp.where(slot_flat == flat_pos[j : j + 1, :], 1.0, 0.0).astype(jnp.bfloat16)
        for c in range(nd):
            hs[j, c] = jnp.dot(pick, h_rows[c], preferred_element_type=jnp.float32).astype(jnp.bfloat16)
        for i in range(nd):
            to = lax.rem(d + i, nd)
            if i or j:
                copy = remote(
                    hs.at[j, to], hr.at[me], h_s.at[j, i], h_r.at[me], dev(dd=to, ee=lax.rem(e + j, ne))
                )
                copy.start()
                sends.append(copy)
    hr[me] = hs[0, d]

    def wait_in(buf, sem, guard=None):
        c = pltpu.make_async_copy(buf, buf, sem)
        if guard is None:
            c.wait()
        else:
            pl.when(guard)(c.wait)

    for i in range(1, nm):
        q = lax.rem(m + i, nm)
        wait_in(cotb.at[q], cb_r.at[q])
    dense = jnp.concatenate([cotb[q] for q in range(nm)], axis=1)
    for j in range(ne):
        block = pack_s(j, dense)
        if j == 0:
            sb[me] = block
            for i in range(1, nd):
                copy = remote(sb.at[me], sb.at[me], db_s.at[i - 1, 0], b_r.at[me], dev(dd=lax.rem(d + i, nd)))
                copy.start()
                sends.append(copy)
        else:
            sbs[j] = block
            copy = remote(sbs.at[j], sb.at[me], xb_s.at[j], b_r.at[me], dev(ee=lax.rem(e + j, ne)))
            copy.start()
            sends.append(copy)

    depth = nd * ne * most
    outs = []

    def nearest(r):
        near = jnp.minimum(m, nm - 1 - m)
        both = m + (r + 1) // 2 * (1 if r % 2 == 0 else -1)
        far = jnp.where(m < nm - 1 - m, m + r - near, m - r + near)
        return jnp.where(r <= 2 * near, both, far)

    def from_partners(q):
        for i in range(1, nd):
            for j in range(ne):
                src = lax.rem(d + i, nd) * ne + j
                wait_in(sa.at[q, src], a_r.at[q, src])

    def send_out(src, dst):
        copy = pltpu.make_async_copy(src, dst, out_sem.at[len(outs)])
        copy.start()
        outs.append(copy)

    def all_hidden():
        for i in range(nd):
            for j in range(ne):
                if i or j:
                    src = lax.rem(d + i, nd) * ne + lax.rem(e + j, ne)
                    wait_in(hr.at[src], h_r.at[src])
        ht[...] = hr[...].reshape(depth, half).T
        send_out(ht, ht_out)

    def product(r):
        q = nearest(r)
        from_partners(q)
        stage[r] = jnp.dot(ht[...], sa[q].reshape(depth, ca), preferred_element_type=jnp.float32)
        send_out(stage.at[r], acc_out.at[q])

    for j in range(1, ne):
        ej = lax.rem(e + j, ne)
        src = d * ne + ej
        wait_in(sa.at[m, src], a_r.at[m, src])
        forward(m, src, m + 1 < nm, m > 0, ej)
        to_partners(m, src, ej)
    for k in range(1, nm):
        below, above = m - k, m + k
        ql, qh = lax.rem(below + nm, nm), lax.rem(above, nm)
        for j in range(ne):
            if k == nm - 1 and j % 2 == 0:
                for r in range(j // 2 * (nm - 1) // 2, nm - 1 if j else (nm - 1) // 2):
                    if r == 0:
                        all_hidden()
                    product(r)
            ej = lax.rem(e + j, ne)
            src = d * ne + ej
            wait_in(sa.at[ql, src], a_r.at[ql, src], below >= 0)
            c = remote(sa.at[ql, src], sa.at[ql, src], up_s.at[ql, ej], a_r.at[ql, src], dev(mm=lax.rem(m + 1, nm)))
            go = (below >= 0) & (m + 1 < nm)
            pl.when(go)(c.start)
            guarded.append((go, c))
            to_partners(ql, src, ej, below >= 0)
            wait_in(sa.at[qh, src], a_r.at[qh, src], above < nm)
            c = remote(sa.at[qh, src], sa.at[qh, src], dn_s.at[qh, ej], a_r.at[qh, src], dev(mm=lax.rem(m + nm - 1, nm)))
            go = (above < nm) & (m > 0)
            pl.when(go)(c.start)
            guarded.append((go, c))
            to_partners(qh, src, ej, above < nm)

    for j in range(1, ne):
        src = d * ne + lax.rem(e + j, ne)
        wait_in(sb.at[src], b_r.at[src])
        for i in range(1, nd):
            copy = remote(sb.at[src], sb.at[src], db_s.at[i - 1, j], b_r.at[src], dev(dd=lax.rem(d + i, nd)))
            copy.start()
            sends.append(copy)

    last = nearest(nm - 1)
    from_partners(last)
    send_out(sa.at[last], last_out)
    for i in range(1, nd):
        for j in range(ne):
            src = lax.rem(d + i, nd) * ne + j
            wait_in(sb.at[src], b_r.at[src])
    send_out(sb, sb_out)
    for i in range(nd):
        for j in range(ne):
            if i or j:
                src = lax.rem(d + i, nd) * ne + lax.rem(e + j, ne)
                wait_in(lbuf.at[src], l_r.at[src])
    total = lbuf[0]
    for k in range(1, nd * ne):
        total = total + lbuf[k]
    load_ref[...] = total

    for c in outs:
        c.wait()
    for c in sends:
        c.wait_send()
    for go, c in guarded:
        pl.when(go)(c.wait_send)


def product_kernel(ht_ref, acc_ref, last_ref, sb_ref, load_ref, out_ref, total_ref, dense):
    q, nm = pl.program_id(0), pl.num_programs(0)
    m = lax.axis_index("mp")
    last = jnp.where(m < nm - 1 - m, nm - 1, 0)
    ca, cb = acc_ref.shape[2], dense.shape[2]

    @pl.when(q == 0)
    def _():
        total_ref[...] = load_ref[0:1, : total_ref.shape[1]]
        cols = jnp.dot(ht_ref[...], sb_ref[...], preferred_element_type=jnp.float32)
        for i in range(dense.shape[0]):
            dense[i] = cols[:, i * cb : (i + 1) * cb]

    @pl.when(q == last)
    def _():
        out_ref[0, :, :ca] = jnp.dot(ht_ref[...], last_ref[...], preferred_element_type=jnp.float32)

    @pl.when(q != last)
    def _():
        out_ref[0, :, :ca] = acc_ref[0]

    out_ref[0, :, ca:] = dense[q]


def fast_body(hidden, cotangent, routes, combine, block_pair, lengths, log_ratio):
    nd, ne, nm = lax.axis_size("dp"), lax.axis_size("expert"), lax.axis_size("mp")
    toks, top, ff = hidden.shape
    width = cotangent.shape[1]
    most = 3 * toks // 4
    cb = width // 4 // LANES * LANES
    ca = width - cb
    half = ff // nd
    srcs = nd * ne
    rows8 = -(-ne // 8) * 8
    dims = (nd, ne, nm, most, ca, cb)
    bf16, f32 = jnp.bfloat16, jnp.float32
    vmem = pl.BlockSpec(memory_space=pltpu.VMEM)
    dma = pltpu.SemaphoreType.DMA
    depth = srcs * most
    hidden_t, done, last, dense, load = pl.pallas_call(
        functools.partial(exchange_kernel, dims),
        out_shape=(
            jax.ShapeDtypeStruct((half, depth), bf16),
            jax.ShapeDtypeStruct((nm, half, ca), f32),
            jax.ShapeDtypeStruct((srcs, most, ca), bf16),
            jax.ShapeDtypeStruct((srcs, most, nm * cb), bf16),
            jax.ShapeDtypeStruct((rows8, LANES), f32),
        ),
        in_specs=[pl.BlockSpec(memory_space=pltpu.HBM)] * 7,
        out_specs=(pl.BlockSpec(memory_space=pltpu.HBM),) * 4 + (vmem,),
        scratch_shapes=[
            pltpu.VMEM((toks, top, ff), bf16),
            pltpu.VMEM(cotangent.shape, bf16),
            pltpu.VMEM((top, toks), jnp.int32),
            pltpu.VMEM((top, toks), f32),
            pltpu.VMEM(block_pair.shape, jnp.int32),
            pltpu.VMEM(lengths.shape, jnp.int32),
            pltpu.VMEM(log_ratio.shape, f32),
            pltpu.VMEM((srcs, most, half), bf16),
            pltpu.VMEM((nm, srcs, most, ca), bf16),
            pltpu.VMEM((srcs, most, nm * cb), bf16),
            pltpu.VMEM((half, depth), bf16),
            pltpu.VMEM((nm - 1, half, ca), f32),
            pltpu.VMEM((ne, nd, most, half), bf16),
            pltpu.VMEM((ne, most, ca), bf16),
            pltpu.VMEM((ne, most, nm * cb), bf16),
            pltpu.VMEM((nm, toks, cb), bf16),
            pltpu.VMEM((srcs, rows8, LANES), f32),
            dma((7,)),
            dma((nm + 2,)),
            dma((ne,)),
            dma((nm, srcs)),
            dma((nm, ne)),
            dma((nm, ne)),
            dma((nm, nd, ne)),
            dma((nm,)),
            dma((nm,)),
            dma((ne,)),
            dma((srcs,)),
            dma((nd, ne)),
            dma((ne, nd)),
            dma((srcs,)),
            dma((srcs,)),
            dma((srcs,)),
        ],
        compiler_params=pltpu.CompilerParams(
            collective_id=0, has_side_effects=True, vmem_limit_bytes=VMEM_MOST
        ),
    )(hidden, cotangent, routes.T, combine.T, block_pair, lengths, log_ratio)
    grad_down, total = pl.pallas_call(
        product_kernel,
        out_shape=(jax.ShapeDtypeStruct((1, half, nm * width), f32), jax.ShapeDtypeStruct((1, ne), f32)),
        grid=(nm,),
        in_specs=[
            pl.BlockSpec((half, depth), lambda q: (0, 0)),
            pl.BlockSpec((1, half, ca), lambda q: (q, 0, 0)),
            pl.BlockSpec((depth, ca), lambda q: (0, 0)),
            pl.BlockSpec((depth, nm * cb), lambda q: (0, 0)),
            pl.BlockSpec((rows8, LANES), lambda q: (0, 0)),
        ],
        out_specs=(
            pl.BlockSpec((1, half, width), lambda q: (0, 0, q)),
            pl.BlockSpec((1, ne), lambda q: (0, 0)),
        ),
        scratch_shapes=[pltpu.VMEM((nm, half, cb), f32)],
        compiler_params=pltpu.CompilerParams(vmem_limit_bytes=VMEM_MOST),
    )(hidden_t, done, last.reshape(depth, ca), dense.reshape(depth, nm * cb), load)
    return grad_down, total.reshape(ne)


def plain_body(hidden, cotangent, routes, combine, block_pair, lengths, log_ratio):
    per_token, within = token_factors(block_pair, lengths, log_ratio, LEN)
    weight = combine * per_token[:, None]
    tok_rows = routes.shape[0]
    route_top = routes.shape[1]
    ff_local = hidden.shape[2]
    groups = lax.axis_size("expert")
    experts = groups * EXP_DEV
    most_rows = 3 * tok_rows // 4
    labels = jnp.arange(experts, dtype=jnp.int32)
    routed = routes[:, :, None] == labels[None, None, :]
    local_load = jnp.sum(jnp.where(routed & within[:, None, None], 1.0, 0.0), axis=(0, 1)).astype(
        jnp.float32
    )
    flat_rows = tok_rows * route_top
    flat_hits = routed.reshape(flat_rows, experts).astype(jnp.int32)
    rank_of = jnp.sum((jnp.cumsum(flat_hits, axis=0) - 1) * flat_hits, axis=1)
    slot_of = routes.reshape(flat_rows) * most_rows + rank_of
    source = (
        jnp.zeros((experts * most_rows,), jnp.int32)
        .at[slot_of]
        .set(jnp.arange(flat_rows, dtype=jnp.int32))
    )
    filled = jnp.zeros((experts * most_rows,), jnp.float32).at[slot_of].set(1.0)
    token_of = source // route_top
    slot_weight = jnp.take(weight.reshape(flat_rows), source) * filled
    packed_h = jnp.take(hidden.reshape(flat_rows, ff_local), source, axis=0).reshape(
        groups, EXP_DEV * most_rows, ff_local
    )
    narrow_s = (
        slot_weight[:, None] * jnp.take(cotangent, token_of, axis=0).astype(jnp.float32)
    ).astype(jnp.bfloat16)
    moved_h, narrow = (
        lax.all_to_all(packed_h, "expert", split_axis=0, concat_axis=0, tiled=True),
        lax.all_to_all(
            narrow_s.reshape(groups, EXP_DEV * most_rows, cotangent.shape[1]),
            "expert",
            split_axis=0,
            concat_axis=0,
            tiled=True,
        ),
    )
    moved_s = lax.all_gather(narrow, "mp", axis=2, tiled=True)
    moved_h = moved_h.reshape(groups, EXP_DEV, most_rows, ff_local)
    moved_s = moved_s.reshape(groups, EXP_DEV, most_rows, moved_s.shape[2])
    products = [
        lax.dot_general(
            moved_h[:, 0],
            moved_s[:, 0],
            (((0, 1), (0, 1)), ((), ())),
            preferred_element_type=jnp.float32,
        )
    ]
    owned = lax.psum_scatter(jnp.stack(products, axis=1), "dp", scatter_dimension=0, tiled=True)
    grad_down = jnp.transpose(owned, (1, 0, 2))
    expert_load = lax.psum(local_load, ("dp", "expert"))
    return (grad_down, expert_load)


def solution(mesh):
    in_specs = (
        P(("dp", "expert"), None, "mp"),
        P(("dp", "expert"), "mp"),
        P(("dp", "expert"), None),
        P(("dp", "expert"), None),
        P(("dp", "expert"), None),
        P(("dp", "expert"), None),
        P(("dp", "expert"), None),
    )
    out_specs = (P("expert", ("mp", "dp"), None), P())

    def body(hidden, cotangent, *rest):
        rows = mesh.shape["dp"] * mesh.shape["expert"] * (3 * hidden.shape[0] // 4)
        bytes_in = 2 * rows * (cotangent.shape[1] * mesh.shape["mp"] + hidden.shape[2])
        run = fast_body if 2 * bytes_in < VMEM_ROOM else plain_body
        return run(hidden, cotangent, *rest)

    return jax.shard_map(body, mesh=mesh, in_specs=in_specs, out_specs=out_specs, check_vma=False)
```

```python
import functools

import jax
import jax.numpy as jnp
from jax import lax
from jax.experimental import pallas as pl
from jax.experimental.pallas import tpu as pltpu
from jax.sharding import PartitionSpec as P

EXP_DEV = 1
LEN = 32
LANES = 128
VMEM_ROOM = 48 * 1024 * 1024
VMEM_MOST = 67043328
MESH = pl.DeviceIdType.MESH


beta_scale = 0.1


def token_factors(block_pair, lengths, log_ratio, block_len):
    blocks = block_pair.shape[1]
    labels = jnp.arange(blocks, dtype=jnp.int32)
    matches = block_pair[:, :, None] == labels[None, None, :]
    by_label = jnp.sum(jnp.where(matches, log_ratio[:, :, None], 0.0), axis=1)
    margin = by_label[:, 0::2] - by_label[:, 1::2]
    pair_coef = beta_scale * jax.nn.sigmoid(-beta_scale * margin)
    owners = block_pair // 2
    pair_ids = jnp.arange(blocks // 2, dtype=jnp.int32)
    picked = owners[:, :, None] == pair_ids[None, None, :]
    block_coef = jnp.sum(jnp.where(picked, pair_coef[:, None, :], 0.0), axis=2)
    block_weight = jnp.where(block_pair % 2 == 0, -block_coef, block_coef)
    position = jnp.arange(block_len, dtype=jnp.int32)
    within = position[None, None, :] < lengths[:, :, None]
    per_token = jnp.where(within, block_weight[:, :, None], 0.0).reshape(-1)
    return per_token, within.reshape(-1)


def exchange_kernel(
    dims, h_hbm, cot_hbm, routes_hbm, combine_hbm, pair_hbm, len_hbm, ratio_hbm,
    ht_out, acc_out, last_out, sb_out, load_ref,
    h_in, cot_ref, routes_ref, combine_ref, pair_ref, len_ref, ratio_ref,
    hr, sa, sb, ht, stage,
    hs, sas, sbs, cotb, lbuf, in_sem, out_sem,
    xa_s, a_r, up_s, dn_s, dd_s, cb_s, cb_r, xb_s, b_r, db_s, h_s, h_r, l_s, l_r,
):
    nd, ne, nm, most, ca, cb = dims
    d, e, m = lax.axis_index("dp"), lax.axis_index("expert"), lax.axis_index("mp")
    toks, top, ff = h_in.shape
    half = ff // nd
    me = d * ne + e

    def dev(dd=None, ee=None, mm=None):
        return {"dp": d if dd is None else dd, "expert": e if ee is None else ee, "mp": m if mm is None else mm}

    def remote(src, dst, ssem, rsem, where):
        return pltpu.make_async_remote_copy(
            src_ref=src, dst_ref=dst, send_sem=ssem, recv_sem=rsem, device_id=where, device_id_type=MESH
        )

    loads = [
        pltpu.make_async_copy(src, dst, in_sem.at[i])
        for i, (src, dst) in enumerate((
            (pair_hbm, pair_ref), (len_hbm, len_ref), (ratio_hbm, ratio_ref), (routes_hbm, routes_ref),
            (combine_hbm, combine_ref), (cot_hbm, cot_ref), (h_hbm, h_in),
        ))
    ]
    for load in loads:
        load.start()
    barrier = pltpu.get_barrier_semaphore()
    peers = [
        dev(dd=lax.rem(d + i, nd), ee=lax.rem(e + j, ne)) for i in range(nd) for j in range(ne) if i or j
    ] + [dev(mm=lax.rem(m + i, nm)) for i in range(1, nm)]
    for peer in peers:
        pl.semaphore_signal(barrier, inc=1, device_id=peer, device_id_type=MESH)

    def ranks(named, n):
        before = lax.broadcasted_iota(jnp.int32, (n, n), 0) < lax.broadcasted_iota(jnp.int32, (n, n), 1)
        rank = jnp.dot(
            jnp.where(named, 1.0, 0.0).astype(jnp.bfloat16),
            jnp.where(before, 1.0, 0.0).astype(jnp.bfloat16),
            preferred_element_type=jnp.float32,
        )
        return jnp.where(named, rank, -1.0)

    for load in loads[:-1]:
        load.wait()

    blocks = pair_ref.shape[1]
    block_len = toks // blocks
    square = (blocks, blocks)
    diagonal = lax.broadcasted_iota(jnp.int32, square, 0) == lax.broadcasted_iota(jnp.int32, square, 1)

    def column(row):
        return jnp.sum(jnp.where(diagonal, row, 0.0), axis=1, keepdims=True)

    pair, ratio = pair_ref[...], ratio_ref[...]
    chosen = lax.rem(pair, 2) == 0
    other_side = jnp.where(chosen, pair + 1, pair - 1)
    is_other = column(pair.astype(jnp.float32)) == other_side.astype(jnp.float32)
    other_ratio = jnp.sum(jnp.where(is_other, column(ratio), 0.0), axis=0, keepdims=True)
    margin = jnp.where(chosen, ratio - other_ratio, other_ratio - ratio)
    coef = beta_scale * (1.0 / (1.0 + jnp.exp(beta_scale * margin)))
    block_weight = column(jnp.where(chosen, -coef, coef))
    token_id = lax.broadcasted_iota(jnp.int32, (blocks, toks), 1)
    place = token_id - block_len * lax.broadcasted_iota(jnp.int32, (blocks, toks), 0)
    inside = (place >= 0) & (place < block_len)
    alive = inside & (place.astype(jnp.float32) < column(len_ref[...].astype(jnp.float32)))
    live = jnp.sum(jnp.where(alive, 1.0, 0.0), axis=0, keepdims=True)
    per_token = jnp.sum(jnp.where(alive, block_weight, 0.0), axis=0, keepdims=True)
    weight = combine_ref[...] * per_token

    rows8 = -(-ne // 8) * 8
    row_id = lax.broadcasted_iota(jnp.int32, (rows8, 1), 0)
    owner = jnp.where(row_id < ne, lax.rem(row_id + e, ne), -1)
    hit0 = routes_ref[0:1, :] == owner
    hit1 = routes_ref[1:2, :] == owner
    named = hit0 | hit1
    tok_rank = ranks(named, toks)
    tok_pos = tok_rank.astype(jnp.int32)
    tok_weight = jnp.where(hit0, weight[0:1, :], 0.0) + jnp.where(hit1, weight[1:2, :], 0.0)
    in_order = (routes_ref[0:1, :] == row_id) | (routes_ref[1:2, :] == row_id)
    counts = jnp.sum(jnp.where(in_order, live, 0.0), axis=1, keepdims=True)
    lanes8 = lax.broadcasted_iota(jnp.int32, (rows8, LANES), 1) == row_id
    lbuf[me] = jnp.broadcast_to(jnp.sum(jnp.where(lanes8, counts, 0.0), axis=0, keepdims=True), (rows8, LANES))

    slot_tok = lax.broadcasted_iota(jnp.int32, (most, toks), 0)
    picks, scales = [], []
    for j in range(ne):
        hit = slot_tok == tok_pos[j : j + 1, :]
        picks.append(jnp.where(hit, 1.0, 0.0).astype(jnp.bfloat16))
        scales.append(jnp.sum(jnp.where(hit, tok_weight[j : j + 1, :], 0.0), axis=1, keepdims=True))

    def pack_s(j, rows):
        rows = jnp.dot(picks[j], rows, preferred_element_type=jnp.float32)
        return (scales[j] * rows).astype(jnp.bfloat16)

    sends = []
    for j in range(ne):
        block = pack_s(j, cot_ref[:, :ca])
        if j == 0:
            sa[m, me] = block
        else:
            sas[j] = block
    cotb[m] = cot_ref[:, ca:]

    pl.semaphore_wait(barrier, len(peers))

    for j in range(1, ne):
        copy = remote(sas.at[j], sa.at[m, me], xa_s.at[j], a_r.at[m, me], dev(ee=lax.rem(e + j, ne)))
        copy.start()
        sends.append(copy)
    for i in range(1, nm):
        copy = remote(cot_ref.at[:, pl.ds(ca, cb)], cotb.at[m], cb_s.at[i], cb_r.at[m], dev(mm=lax.rem(m + i, nm)))
        copy.start()
        sends.append(copy)
    n = 0
    for i in range(nd):
        for j in range(ne):
            if i or j:
                copy = remote(
                    lbuf.at[me], lbuf.at[me], l_s.at[n], l_r.at[me], dev(dd=lax.rem(d + i, nd), ee=lax.rem(e + j, ne))
                )
                copy.start()
                sends.append(copy)
                n += 1

    guarded = []

    def forward(q, src, up, down, ek):
        block = sa.at[q, src]
        cu = remote(block, block, up_s.at[q, ek], a_r.at[q, src], dev(mm=lax.rem(m + 1, nm)))
        cd = remote(block, block, dn_s.at[q, ek], a_r.at[q, src], dev(mm=lax.rem(m + nm - 1, nm)))

        @pl.when(up)
        def _():
            cu.start()

        @pl.when(down)
        def _():
            cd.start()

        guarded.append((up, cu))
        guarded.append((down, cd))

    def to_partners(q, src, ek, guard=None):
        for i in range(1, nd):
            c = remote(sa.at[q, src], sa.at[q, src], dd_s.at[q, i - 1, ek], a_r.at[q, src], dev(dd=lax.rem(d + i, nd)))
            if guard is None:
                c.start()
                sends.append(c)
            else:
                pl.when(guard)(c.start)
                guarded.append((guard, c))

    forward(m, me, m + 1 < nm, m > 0, e)
    to_partners(m, me, e)

    slot_flat = lax.broadcasted_iota(jnp.int32, (most, 2 * toks), 0)
    gap = lax.broadcasted_iota(jnp.int32, (toks, 2 * toks), 1) - 2 * lax.broadcasted_iota(
        jnp.int32, (toks, 2 * toks), 0
    )
    flat_pos = -1.0
    for k, hit in enumerate((hit0, hit1)):
        spread = jnp.where(gap == k, 1.0, 0.0).astype(jnp.bfloat16)
        value = jnp.where(hit, tok_rank + 1.0, 0.0)
        high = jnp.floor(value * (1.0 / 16.0))
        for part, unit in ((high, 16.0), (value - 16.0 * high, 1.0)):
            flat_pos += unit * jnp.dot(part.astype(jnp.bfloat16), spread, preferred_element_type=jnp.float32)
    flat_pos = flat_pos.astype(jnp.int32)
    loads[-1].wait()
    flat = (2 * toks, half)
    h_rows = [h_in[:, :, c * half : (c + 1) * half].reshape(flat) for c in range(nd)]
    for j in [*range(1, ne), 0]:
        pick = jnp.where(slot_flat == flat_pos[j : j + 1, :], 1.0, 0.0).astype(jnp.bfloat16)
        for c in range(nd):
            hs[j, c] = jnp.dot(pick, h_rows[c], preferred_element_type=jnp.float32).astype(jnp.bfloat16)
        for i in range(nd):
            to = lax.rem(d + i, nd)
            if i or j:
                copy = remote(
                    hs.at[j, to], hr.at[me], h_s.at[j, i], h_r.at[me], dev(dd=to, ee=lax.rem(e + j, ne))
                )
                copy.start()
                sends.append(copy)
    hr[me] = hs[0, d]

    def wait_in(buf, sem, guard=None):
        c = pltpu.make_async_copy(buf, buf, sem)
        if guard is None:
            c.wait()
        else:
            pl.when(guard)(c.wait)

    for i in range(1, nm):
        q = lax.rem(m + i, nm)
        wait_in(cotb.at[q], cb_r.at[q])
    dense = jnp.concatenate([cotb[q] for q in range(nm)], axis=1)
    for j in range(ne):
        block = pack_s(j, dense)
        if j == 0:
            sb[me] = block
            for i in range(1, nd):
                copy = remote(sb.at[me], sb.at[me], db_s.at[i - 1, 0], b_r.at[me], dev(dd=lax.rem(d + i, nd)))
                copy.start()
                sends.append(copy)
        else:
            sbs[j] = block
            copy = remote(sbs.at[j], sb.at[me], xb_s.at[j], b_r.at[me], dev(ee=lax.rem(e + j, ne)))
            copy.start()
            sends.append(copy)

    depth = nd * ne * most
    outs = []

    def nearest(r):
        near = jnp.minimum(m, nm - 1 - m)
        both = m + (r + 1) // 2 * (1 if r % 2 == 0 else -1)
        far = jnp.where(m < nm - 1 - m, m + r - near, m - r + near)
        return jnp.where(r <= 2 * near, both, far)

    def from_partners(q):
        for i in range(1, nd):
            for j in range(ne):
                src = lax.rem(d + i, nd) * ne + j
                wait_in(sa.at[q, src], a_r.at[q, src])

    def send_out(src, dst):
        copy = pltpu.make_async_copy(src, dst, out_sem.at[len(outs)])
        copy.start()
        outs.append(copy)

    def all_hidden():
        for i in range(nd):
            for j in range(ne):
                if i or j:
                    src = lax.rem(d + i, nd) * ne + lax.rem(e + j, ne)
                    wait_in(hr.at[src], h_r.at[src])
        ht[...] = hr[...].reshape(depth, half).T
        send_out(ht, ht_out)

    def product(r):
        q = nearest(r)
        from_partners(q)
        stage[r] = jnp.dot(ht[...], sa[q].reshape(depth, ca), preferred_element_type=jnp.float32)
        send_out(stage.at[r], acc_out.at[q])

    for j in range(1, ne):
        ej = lax.rem(e + j, ne)
        src = d * ne + ej
        wait_in(sa.at[m, src], a_r.at[m, src])
        forward(m, src, m + 1 < nm, m > 0, ej)
        to_partners(m, src, ej)
    for k in range(1, nm):
        below, above = m - k, m + k
        ql, qh = lax.rem(below + nm, nm), lax.rem(above, nm)
        for j in range(ne):
            if k == nm - 1 and j % 2 == 0:
                for r in range(j // 2 * (nm - 1) // 2, nm - 1 if j else (nm - 1) // 2):
                    if r == 0:
                        all_hidden()
                    product(r)
            ej = lax.rem(e + j, ne)
            src = d * ne + ej
            wait_in(sa.at[ql, src], a_r.at[ql, src], below >= 0)
            c = remote(sa.at[ql, src], sa.at[ql, src], up_s.at[ql, ej], a_r.at[ql, src], dev(mm=lax.rem(m + 1, nm)))
            go = (below >= 0) & (m + 1 < nm)
            pl.when(go)(c.start)
            guarded.append((go, c))
            to_partners(ql, src, ej, below >= 0)
            wait_in(sa.at[qh, src], a_r.at[qh, src], above < nm)
            c = remote(sa.at[qh, src], sa.at[qh, src], dn_s.at[qh, ej], a_r.at[qh, src], dev(mm=lax.rem(m + nm - 1, nm)))
            go = (above < nm) & (m > 0)
            pl.when(go)(c.start)
            guarded.append((go, c))
            to_partners(qh, src, ej, above < nm)

    for j in range(1, ne):
        src = d * ne + lax.rem(e + j, ne)
        wait_in(sb.at[src], b_r.at[src])
        for i in range(1, nd):
            copy = remote(sb.at[src], sb.at[src], db_s.at[i - 1, j], b_r.at[src], dev(dd=lax.rem(d + i, nd)))
            copy.start()
            sends.append(copy)

    last = nearest(nm - 1)
    from_partners(last)
    send_out(sa.at[last], last_out)
    for i in range(1, nd):
        for j in range(ne):
            src = lax.rem(d + i, nd) * ne + j
            wait_in(sb.at[src], b_r.at[src])
    send_out(sb, sb_out)
    for i in range(nd):
        for j in range(ne):
            if i or j:
                src = lax.rem(d + i, nd) * ne + lax.rem(e + j, ne)
                wait_in(lbuf.at[src], l_r.at[src])
    total = lbuf[0]
    for k in range(1, nd * ne):
        total = total + lbuf[k]
    load_ref[...] = total

    for c in outs:
        c.wait()
    for c in sends:
        c.wait_send()
    for go, c in guarded:
        pl.when(go)(c.wait_send)


def product_kernel(nm, ht_ref, acc_ref, last_ref, sb_ref, load_ref, out_ref, total_ref):
    m = lax.axis_index("mp")
    last = jnp.where(m < nm - 1 - m, nm - 1, 0)
    ca, cb = acc_ref.shape[2], sb_ref.shape[1] // nm
    width = ca + cb
    total_ref[...] = load_ref[0:1, : total_ref.shape[1]]
    tail = jnp.dot(ht_ref[...], last_ref[...], preferred_element_type=jnp.float32)
    cols = jnp.dot(ht_ref[...], sb_ref[...], preferred_element_type=jnp.float32)
    for q in range(nm):
        out_ref[0, :, q * width + ca : (q + 1) * width] = cols[:, q * cb : (q + 1) * cb]
        out_ref[0, :, q * width : q * width + ca] = jnp.where(last == q, tail, acc_ref[q])


def fast_body(hidden, cotangent, routes, combine, block_pair, lengths, log_ratio):
    nd, ne, nm = lax.axis_size("dp"), lax.axis_size("expert"), lax.axis_size("mp")
    toks, top, ff = hidden.shape
    width = cotangent.shape[1]
    most = 3 * toks // 4
    cb = width // 4 // LANES * LANES
    ca = width - cb
    half = ff // nd
    srcs = nd * ne
    rows8 = -(-ne // 8) * 8
    dims = (nd, ne, nm, most, ca, cb)
    bf16, f32 = jnp.bfloat16, jnp.float32
    vmem = pl.BlockSpec(memory_space=pltpu.VMEM)
    dma = pltpu.SemaphoreType.DMA
    depth = srcs * most
    hidden_t, done, last, dense, load = pl.pallas_call(
        functools.partial(exchange_kernel, dims),
        out_shape=(
            jax.ShapeDtypeStruct((half, depth), bf16),
            jax.ShapeDtypeStruct((nm, half, ca), f32),
            jax.ShapeDtypeStruct((srcs, most, ca), bf16),
            jax.ShapeDtypeStruct((srcs, most, nm * cb), bf16),
            jax.ShapeDtypeStruct((rows8, LANES), f32),
        ),
        in_specs=[pl.BlockSpec(memory_space=pltpu.HBM)] * 7,
        out_specs=(pl.BlockSpec(memory_space=pltpu.HBM),) * 4 + (vmem,),
        scratch_shapes=[
            pltpu.VMEM((toks, top, ff), bf16),
            pltpu.VMEM(cotangent.shape, bf16),
            pltpu.VMEM((top, toks), jnp.int32),
            pltpu.VMEM((top, toks), f32),
            pltpu.VMEM(block_pair.shape, jnp.int32),
            pltpu.VMEM(lengths.shape, jnp.int32),
            pltpu.VMEM(log_ratio.shape, f32),
            pltpu.VMEM((srcs, most, half), bf16),
            pltpu.VMEM((nm, srcs, most, ca), bf16),
            pltpu.VMEM((srcs, most, nm * cb), bf16),
            pltpu.VMEM((half, depth), bf16),
            pltpu.VMEM((nm - 1, half, ca), f32),
            pltpu.VMEM((ne, nd, most, half), bf16),
            pltpu.VMEM((ne, most, ca), bf16),
            pltpu.VMEM((ne, most, nm * cb), bf16),
            pltpu.VMEM((nm, toks, cb), bf16),
            pltpu.VMEM((srcs, rows8, LANES), f32),
            dma((7,)),
            dma((nm + 2,)),
            dma((ne,)),
            dma((nm, srcs)),
            dma((nm, ne)),
            dma((nm, ne)),
            dma((nm, nd, ne)),
            dma((nm,)),
            dma((nm,)),
            dma((ne,)),
            dma((srcs,)),
            dma((nd, ne)),
            dma((ne, nd)),
            dma((srcs,)),
            dma((srcs,)),
            dma((srcs,)),
        ],
        compiler_params=pltpu.CompilerParams(
            collective_id=0, has_side_effects=True, vmem_limit_bytes=VMEM_MOST
        ),
    )(hidden, cotangent, routes.T, combine.T, block_pair, lengths, log_ratio)
    steps = next(n for n in (4, 2, 1) if half % (16 * n) == 0 or n == 1)
    rows = half // steps
    grad_down, total = pl.pallas_call(
        functools.partial(product_kernel, nm),
        out_shape=(jax.ShapeDtypeStruct((1, half, nm * width), f32), jax.ShapeDtypeStruct((1, ne), f32)),
        grid=(steps,),
        in_specs=[
            pl.BlockSpec((rows, depth), lambda i: (i, 0)),
            pl.BlockSpec((nm, rows, ca), lambda i: (0, i, 0)),
            pl.BlockSpec((depth, ca), lambda i: (0, 0)),
            pl.BlockSpec((depth, nm * cb), lambda i: (0, 0)),
            pl.BlockSpec((rows8, LANES), lambda i: (0, 0)),
        ],
        out_specs=(
            pl.BlockSpec((1, rows, nm * width), lambda i: (0, i, 0)),
            pl.BlockSpec((1, ne), lambda i: (0, 0)),
        ),
        compiler_params=pltpu.CompilerParams(vmem_limit_bytes=VMEM_MOST),
    )(hidden_t, done, last.reshape(depth, ca), dense.reshape(depth, nm * cb), load)
    return grad_down, total.reshape(ne)


def plain_body(hidden, cotangent, routes, combine, block_pair, lengths, log_ratio):
    per_token, within = token_factors(block_pair, lengths, log_ratio, LEN)
    weight = combine * per_token[:, None]
    tok_rows = routes.shape[0]
    route_top = routes.shape[1]
    ff_local = hidden.shape[2]
    groups = lax.axis_size("expert")
    experts = groups * EXP_DEV
    most_rows = 3 * tok_rows // 4
    labels = jnp.arange(experts, dtype=jnp.int32)
    routed = routes[:, :, None] == labels[None, None, :]
    local_load = jnp.sum(jnp.where(routed & within[:, None, None], 1.0, 0.0), axis=(0, 1)).astype(
        jnp.float32
    )
    flat_rows = tok_rows * route_top
    flat_hits = routed.reshape(flat_rows, experts).astype(jnp.int32)
    rank_of = jnp.sum((jnp.cumsum(flat_hits, axis=0) - 1) * flat_hits, axis=1)
    slot_of = routes.reshape(flat_rows) * most_rows + rank_of
    source = (
        jnp.zeros((experts * most_rows,), jnp.int32)
        .at[slot_of]
        .set(jnp.arange(flat_rows, dtype=jnp.int32))
    )
    filled = jnp.zeros((experts * most_rows,), jnp.float32).at[slot_of].set(1.0)
    token_of = source // route_top
    slot_weight = jnp.take(weight.reshape(flat_rows), source) * filled
    packed_h = jnp.take(hidden.reshape(flat_rows, ff_local), source, axis=0).reshape(
        groups, EXP_DEV * most_rows, ff_local
    )
    narrow_s = (
        slot_weight[:, None] * jnp.take(cotangent, token_of, axis=0).astype(jnp.float32)
    ).astype(jnp.bfloat16)
    moved_h, narrow = (
        lax.all_to_all(packed_h, "expert", split_axis=0, concat_axis=0, tiled=True),
        lax.all_to_all(
            narrow_s.reshape(groups, EXP_DEV * most_rows, cotangent.shape[1]),
            "expert",
            split_axis=0,
            concat_axis=0,
            tiled=True,
        ),
    )
    moved_s = lax.all_gather(narrow, "mp", axis=2, tiled=True)
    moved_h = moved_h.reshape(groups, EXP_DEV, most_rows, ff_local)
    moved_s = moved_s.reshape(groups, EXP_DEV, most_rows, moved_s.shape[2])
    products = [
        lax.dot_general(
            moved_h[:, 0],
            moved_s[:, 0],
            (((0, 1), (0, 1)), ((), ())),
            preferred_element_type=jnp.float32,
        )
    ]
    owned = lax.psum_scatter(jnp.stack(products, axis=1), "dp", scatter_dimension=0, tiled=True)
    grad_down = jnp.transpose(owned, (1, 0, 2))
    expert_load = lax.psum(local_load, ("dp", "expert"))
    return (grad_down, expert_load)


def solution(mesh):
    in_specs = (
        P(("dp", "expert"), None, "mp"),
        P(("dp", "expert"), "mp"),
        P(("dp", "expert"), None),
        P(("dp", "expert"), None),
        P(("dp", "expert"), None),
        P(("dp", "expert"), None),
        P(("dp", "expert"), None),
    )
    out_specs = (P("expert", ("mp", "dp"), None), P())

    def body(hidden, cotangent, *rest):
        rows = mesh.shape["dp"] * mesh.shape["expert"] * (3 * hidden.shape[0] // 4)
        bytes_in = 2 * rows * (cotangent.shape[1] * mesh.shape["mp"] + hidden.shape[2])
        run = fast_body if 2 * bytes_in < VMEM_ROOM else plain_body
        return run(hidden, cotangent, *rest)

    return jax.shard_map(body, mesh=mesh, in_specs=in_specs, out_specs=out_specs, check_vma=False)
```
